32 devices in a mesh: row: 8 (over z, x), col: 4 (over y, core).
Axes of the slice: x: 2, y: 2, z: 4, core: 2. Of those that a mesh axis runs over, the one named last changes fastest.
Arguments:
- krylov_basis: float32 [4, 2, 3, 128, 128, 256], P(None, None, None, 'col', 'row'), may hold values from -50 to 50
- susceptibility: float32 [128, 128, 256], P('col', 'row'), may hold values from 0.1 to 1
- green_spectra: bfloat16 [6, 256, 256, 512], P(None, None, 'col', 'row'), may hold values from -3 to 3, as said below
Outputs:
- projections: float32 [4, 2, 2], replicated
- next_block: float32 [2, 3, 128, 128, 256], P(None, None, 'col', 'row')
- block_factor: float32 [2, 2], replicated
The draws below stay inside these ranges and needn't reach their ends.
Inputs may be any that keep to these rules, and one draw needn't show every extreme that they name: `green_spectra`: each of the six arrays is even on the padded grid: its value at (a, b, c) equals its value at ((-a) mod 256, (-b) mod 256, (-c) mod 512).
All inputs are finite; a program needn't handle non-finite values.
Results may differ from the reference program's by a relative error of at most 0.0003.
Values sent between devices are 32-bit elements; how exact they have to be, the bound alone decides.
A program may use at most 192 MiB of HBM per device.

```python
import math
import jax
import jax.numpy as jnp
from jax import lax

GX = 256
GY = 128
GZ = 128
NB = 4


def draw_krylov_basis(key, part):
    shared = jnp.clip(jax.random.normal(jax.random.fold_in(key, 12), (2, 3, GZ, GY, GX), jnp.float32), -6.0, 6.0)
    depths = (jnp.arange(GZ, dtype=jnp.float32) + 0.5) / GZ
    across = (jnp.arange(GY, dtype=jnp.float32) + 0.5) / GY
    envelope = (0.3 + depths[:, None] + across[None, :])[:, :, None]
    own = jnp.clip(jax.random.normal(jax.random.fold_in(key, 11), (NB, 2, 3, GZ, GY, GX), jnp.float32), -6.0, 6.0)
    return (own + shared) * (envelope * math.sqrt(0.5))


def draw_green_spectra(key, part):

    def one_entry(entry_key):
        raw = jnp.clip(jax.random.normal(entry_key, (2 * GZ, 2 * GY, 2 * GX), jnp.float32), -6.0, 6.0)
        mirrored = jnp.roll(jnp.flip(raw), (1, 1, 1), axis=(0, 1, 2))
        return (0.25 * (raw + mirrored)).astype(jnp.bfloat16)
    entry_keys = jax.random.split(jax.random.fold_in(key, 21), 6)
    return lax.map(one_entry, entry_keys)


def block_scale(stream_key, extent, cuts, low, high):
    def one(dim, blocks):
        draws = jax.random.uniform(jax.random.fold_in(jax.random.fold_in(stream_key, 6), dim), (blocks,), jnp.float32, low / len(cuts), high / len(cuts))
        return jnp.repeat(jnp.exp(draws), extent[dim] // blocks).reshape((-1,) + (1,) * (len(extent) - dim - 1))

    factor_of = one(*cuts[0])
    for cut in cuts[1:]:
        factor_of = factor_of * one(*cut)
    return factor_of


def setup_inputs(seed: int = 0) -> dict:
    key_list = jax.random.split(jax.random.key(seed), 4)
    return {
        "krylov_basis": draw_krylov_basis(jax.random.fold_in(key_list[3], 71), 0),
        "susceptibility": jnp.clip(jnp.exp(math.log(1.0) - 2.3025851 * jax.random.uniform(key_list[1], (GZ, GY, GX), jnp.float32) ** block_scale(key_list[1], (GZ, GY, GX), ((0, 4), (1, 8)), -0.2, 0.2)), 0.1, 1.0),
        "green_spectra": draw_green_spectra(jax.random.fold_in(key_list[3], 71), 0),
    }


highest = lax.Precision.HIGHEST
tensor_pairs = ((0, 3, 4), (3, 1, 5), (4, 5, 2))

def convolve(field, green_spectra):
    padded_shape = (2 * GZ, 2 * GY, 2 * GX)
    half_kernel = green_spectra[:, :, :, :GX + 1].astype(jnp.float32)
    spectra = jnp.fft.rfftn(field, s=padded_shape, axes=(1, 2, 3))
    results = []
    for member in range(3):
        chosen = tensor_pairs[member]
        mixed = half_kernel[chosen[0]] * spectra[0] + half_kernel[chosen[1]] * spectra[1] + half_kernel[chosen[2]] * spectra[2]
        full_field = jnp.fft.irfftn(mixed, s=padded_shape, axes=(0, 1, 2))
        results.append(full_field[:GZ, :GY, :GX])
    return jnp.stack(results)

def reference(krylov_basis, susceptibility, green_spectra):
    latest = krylov_basis[NB - 1]
    response = jnp.stack([convolve(latest[0], green_spectra), convolve(latest[1], green_spectra)])
    image = latest - susceptibility[None, None] * response
    entry_count = 3.0 * GX * GY * GZ
    flat_basis = krylov_basis.reshape(2 * NB, -1)
    flat_image = image.reshape(2, -1)
    coefficients = jnp.dot(flat_basis, flat_image.T, precision=highest) / entry_count
    projected = flat_image - jnp.dot(coefficients.T, flat_basis, precision=highest)
    gram = jnp.dot(projected, projected.T, precision=highest) / entry_count
    lead_norm = jnp.sqrt(gram[0, 0] + 1e-06)
    cross_term = gram[0, 1] / lead_norm
    tail_norm = jnp.sqrt(gram[1, 1] - cross_term * cross_term + 1e-06)
    first_column = projected[0] / lead_norm
    second_column = (projected[1] - cross_term * first_column) / tail_norm
    next_block = jnp.stack([first_column, second_column]).reshape(image.shape)
    block_factor = jnp.stack([jnp.stack([lead_norm, cross_term]), jnp.stack([jnp.zeros_like(lead_norm), tail_norm])])
    return (coefficients.reshape(NB, 2, 2), next_block, block_factor)
```

```python
import math

import jax
import jax.numpy as jnp
from jax import lax
from jax.sharding import PartitionSpec as P

fast = lax.Precision.HIGH
tensor_pairs = ((0, 3, 4), (3, 1, 5), (4, 5, 2))


def twiddle(count_in, count_out, period, orient, factor):
    row_index = lax.broadcasted_iota(jnp.int32, (count_in, count_out), 0)
    col_index = lax.broadcasted_iota(jnp.int32, (count_in, count_out), 1)
    phases = row_index * col_index % period
    angles = phases.astype(jnp.float32) * (2.0 * math.pi / period)
    cosine = jnp.cos(angles) * factor
    sines = jnp.sin(angles) * (orient * factor)
    return jnp.stack([jnp.stack([cosine, sines]), jnp.stack([-sines, cosine])])


def exchange_rows(blocks):
    return lax.all_to_all(blocks, "row", split_axis=0, concat_axis=0, tiled=True)


def exchange_cols(blocks):
    return lax.all_to_all(blocks, "col", split_axis=0, concat_axis=0, tiled=True)


def forward(source, table_x, table_y, table_z):
    local_z, local_y = source.shape[1:3]
    row_count, part_x = table_x.shape[-2:]
    col_count, part_y = table_y.shape[-2:]
    spectra = jnp.einsum("rzyx,rsxdl->dsyzl", source, table_x, precision=fast)
    spectra = spectra.reshape(row_count, 2, local_y, local_z * part_x)
    spectra = exchange_rows(spectra)
    spectra = spectra.transpose(1, 0, 2, 3).reshape(2, row_count * local_y, local_z, part_x)
    spectra = jnp.einsum("ryzl,rsyeq->eszql", spectra, table_y, precision=fast)
    spectra = spectra.reshape(col_count, 2, local_z, part_y * part_x)
    spectra = exchange_cols(spectra)
    spectra = spectra.transpose(1, 0, 2, 3).reshape(2, col_count * local_z, part_y * part_x)
    return jnp.einsum("rzb,rszk->skb", spectra, table_z, precision=fast)


def backward(spectra, back_x, back_y, back_z):
    row_count, part_x = back_x.shape[2:4]
    col_count, part_y, width = back_y.shape[2:]
    spectra = jnp.einsum("rkb,rskz->szb", spectra, back_z, precision=fast)
    local_z = spectra.shape[1] // col_count
    spectra = spectra.reshape(2, col_count, local_z, part_y * part_x).transpose(1, 0, 2, 3)
    spectra = exchange_cols(spectra)
    spectra = spectra.reshape(col_count, 2, local_z, part_y, part_x)
    spectra = jnp.einsum("erzql,rseqy->syzl", spectra, back_y, precision=fast)
    local_y = width // row_count
    spectra = spectra.reshape(2, row_count, local_y, local_z * part_x).transpose(1, 0, 2, 3)
    spectra = exchange_rows(spectra)
    spectra = spectra.reshape(row_count, 2, local_y, local_z, part_x)
    return jnp.einsum("dryzl,rsdlx->szyx", spectra, back_x, precision=fast)


def convolve(source, green_spectra):
    row_count = lax.axis_size("row")
    col_count = lax.axis_size("col")
    width_x = 2 * source.shape[-1]
    width_y = 2 * source.shape[-2] * row_count
    width_z = 2 * source.shape[-3] * col_count
    part_x = width_x // row_count
    part_y = width_y // col_count
    half_x, half_y, half_z = width_x // 2, width_y // 2, width_z // 2
    table_x = twiddle(half_x, width_x, width_x, -1.0, 1.0).reshape(2, 2, half_x, row_count, part_x)
    table_y = twiddle(half_y, width_y, width_y, -1.0, 1.0).reshape(2, 2, half_y, col_count, part_y)
    table_z = twiddle(half_z, width_z, width_z, -1.0, 1.0)
    spectra = [forward(source[:, c], table_x, table_y, table_z) for c in range(3)]
    coupling = green_spectra.astype(jnp.float32).reshape(6, width_z, part_y * part_x)
    back_z = twiddle(width_z, half_z, width_z, 1.0, 1.0)
    back_y = twiddle(width_y, half_y, width_y, 1.0, 1.0).reshape(2, 2, col_count, part_y, half_y)
    scaling = 1.0 / (width_x * width_y * width_z)
    back_x = twiddle(width_x, half_x, width_x, 1.0, scaling).reshape(2, 2, row_count, part_x, half_x)
    result = []
    for member in range(3):
        chosen = tensor_pairs[member]
        total = coupling[chosen[0]] * spectra[0]
        total = total + coupling[chosen[1]] * spectra[1]
        total = total + coupling[chosen[2]] * spectra[2]
        result.append(backward(total, back_x, back_y, back_z))
    return result


def total_over_devices(partial):
    return jnp.sum(lax.all_gather(partial, ("row", "col")), axis=0)


def per_device(krylov_basis, susceptibility, green_spectra):
    blocks = krylov_basis.shape[0]
    latest = krylov_basis[-1]
    response = convolve(latest, green_spectra)
    image = [latest[:, c] - susceptibility[None] * response[c] for c in range(3)]
    image = jnp.stack(image, axis=1)
    entry_count = 3.0 * susceptibility.size * lax.axis_size("row") * lax.axis_size("col")
    basis = krylov_basis.reshape((2 * blocks,) + image.shape[1:])
    local_coeffs = jnp.stack(
        [jnp.sum(basis * image[j][None], axis=(1, 2, 3, 4)) for j in range(2)], axis=1
    )
    coefficients = total_over_devices(local_coeffs / entry_count)
    projected = []
    for j in range(2):
        column = image[j]
        for a in range(2 * blocks):
            column = column - coefficients[a, j] * basis[a]
        projected.append(column)
    g00 = jnp.sum(projected[0] * projected[0])
    g01 = jnp.sum(projected[0] * projected[1])
    g11 = jnp.sum(projected[1] * projected[1])
    gram = total_over_devices(jnp.stack([g00, g01, g11]) / entry_count)
    lead_norm = jnp.sqrt(gram[0] + 1e-06)
    cross_term = gram[1] / lead_norm
    tail_norm = jnp.sqrt(gram[2] - cross_term * cross_term + 1e-06)
    first_column = projected[0] / lead_norm
    second_column = (projected[1] - cross_term * first_column) / tail_norm
    next_block = jnp.stack([first_column, second_column])
    block_factor = jnp.stack(
        [jnp.stack([lead_norm, cross_term]), jnp.stack([jnp.zeros_like(lead_norm), tail_norm])]
    )
    return (coefficients.reshape(blocks, 2, 2), next_block, block_factor)


def solution(mesh):
    in_specs = (
        P(None, None, None, "col", "row", None),
        P("col", "row", None),
        P(None, None, "col", "row"),
    )
    out_specs = (P(), P(None, None, "col", "row", None), P())
    return jax.shard_map(
        per_device, mesh=mesh, in_specs=in_specs, out_specs=out_specs, check_vma=False
    )
```
